32 devices in a mesh: ga: 1, ea: 32 (over z, y, x, core).
Axes of the slice: x: 2, y: 2, z: 4, core: 2. Of those that a mesh axis runs over, the one named last changes fastest.
Arguments:
- tokens: bfloat16 [256, 7168], P(('ga', 'ea')), may hold values from -6 to 6
- route_slot: int32 [256, 2], P(('ga', 'ea')), may hold values from 0 to 3, all different within a row; in each aligned block of 8 rows (0 to 7, 8 to 15, ...) at most 8 rows name the same one
- gates: float32 [256, 2], P(('ga', 'ea')), may hold values from 0.2 to 1
- gate_up: bfloat16 [32, 7168, 512], P('ea'), may hold values from -0.0625 to 0.0625
- down: bfloat16 [32, 256, 7168], P('ea'), may hold values from -0.125 to 0.125
Outputs:
- mixed: bfloat16 [256, 7168], P(('ga', 'ea'))
The draws below stay inside these ranges and needn't reach their ends.
Inputs may be any that keep to these rules, and one draw needn't show every extreme that they name: `route_slot`: each token names 2 different replicas. Among the tokens of one device no replica is named more than 8 times, and some device names some replica exactly 8 times.
All inputs are finite; a program needn't handle non-finite values.
Results may differ from the reference program's by a relative error of at most 0.0087.
Values may be sent and summed in bfloat16 or wider, within the bound.
No kernel may reach another device: no remote copies, remote signals or barrier semaphores. Data moves between devices by JAX's collectives and lax.ppermute only.
A program may use at most 64 MiB of HBM per device.

```python
import math
import jax
import jax.numpy as jnp
import numpy as np
from jax import lax

D = 7168
FF = 2048
TP = 8
TOPK = 2
TOK_DEV = 8
HS = 256
SLOTS = 4
CAP = 8
TOKENS = 256
N_EA = 32


def levels(own_key, shape, cuts, smallest, high):
    loudness = 1.0
    for dim, shards_of in cuts:
        heights = jax.random.uniform(jax.random.fold_in(jax.random.fold_in(own_key, 6), dim), (shards_of,), jnp.float32, smallest / len(cuts), high / len(cuts))
        loudness = loudness * jnp.repeat(jnp.exp(heights), shape[dim] // shards_of).reshape((-1,) + (1,) * (len(shape) - 1 - dim))
    return loudness


def routed_block(own_key, own, number, rows, number_of, top, reach, slope):
    sequence = jax.random.permutation(own_key, number_of)
    crowded, ordinary = shares(number_of, rows * top, reach, slope, True), shares(number_of, rows * top, reach, slope, False)
    places = jnp.arange(number_of)

    def named(sizes, offset_by):
        used = int((sizes > 0).sum())
        fixed = max(1, used // 4)
        passed = fixed + (places - fixed + offset_by * (used - fixed)) % max(1, number_of - fixed)
        return jnp.zeros((number_of,), jnp.int32).at[sequence[jnp.where(places < fixed, places, passed)]].set(jnp.asarray(sizes, jnp.int32))

    sizes = jnp.where(number % 4 == 0, named(crowded, number // 4), named(ordinary, number - number // 4 - 1))
    mixed = jax.random.permutation(jax.random.fold_in(own, 3), number_of)
    donor, receiver = mixed[0:number_of // 2 * 2:2], mixed[1:number_of // 2 * 2:2]
    slack = jnp.minimum(sizes[donor] - 1, reach - sizes[receiver]) // 2
    slack = jnp.where((donor == sequence[0]) | (receiver == sequence[0]) | (sizes[receiver] == 0), 0, jnp.maximum(slack, 0))
    passed = jax.random.randint(jax.random.fold_in(own, 4), (number_of // 2,), 0, 1 << 20) % (slack + 1)
    sizes = sizes.at[donor].add(-passed).at[receiver].add(passed)
    items = jnp.searchsorted(jnp.cumsum(sizes), jnp.arange(rows * top), side="right").astype(jnp.int32)
    grid = items.reshape(top, rows).T
    grid = grid[jax.random.permutation(jax.random.fold_in(own, 1), rows)]
    offset_by = jax.random.randint(jax.random.fold_in(own, 2), (rows, 1), 0, top)
    return jnp.take_along_axis(grid, (jnp.arange(top)[None, :] + offset_by) % top, axis=1)


def shares(number_of, total, bound, slope, full):
    weights = [(1 << 20) // math.isqrt(standing ** slope) + 1 for standing in range(1, number_of + 1)]
    largest = bound if full else min(bound, max(-(-total // number_of), total * weights[0] // sum(weights)))
    least = 1 if total - largest >= number_of - 1 else 0
    given, surplus = [largest] + [least] * (number_of - 1), total - largest - least * (number_of - 1)
    while surplus > 0:
        candidates = [i for i in range(1, number_of) if given[i] < largest] or [i for i in range(1, number_of) if given[i] < bound]
        mass, left = sum([weights[i] for i in candidates]), surplus
        for i in candidates:
            more = min(bound - given[i], max(1, left * weights[i] // mass), surplus)
            given[i] = given[i] + more
            surplus = surplus - more
    return np.array(given)


def normal_values(rng, extent, spread, limit, cuts=(), held_as=jnp.bfloat16):
    loudness = levels(rng, extent, cuts, -0.22, 0.18) if cuts else 1.0
    values = jax.random.normal(rng, extent, jnp.float32) * spread * loudness
    return jnp.minimum(jnp.maximum(values, -limit), limit).astype(held_as)


def setup_inputs(seed: int = 0, part: int = 0) -> dict:
    key_of = jax.random.split(jax.random.key(seed), 6)
    part_splits = jax.random.split(jax.random.fold_in(key_of[5], part), 6)
    tokens = normal_values(part_splits[0], (TOKENS, D), 1.0, 6.0, ((0, 32),))
    route_slot_keys = jax.random.split(jax.random.fold_in(part_splits[1], 1), TOKENS // TOK_DEV)
    route_slot_turns = jax.random.permutation(jax.random.fold_in(part_splits[1], 3), TOKENS // TOK_DEV)
    route_slot = jax.vmap(lambda own, number: routed_block(jax.random.fold_in(part_splits[1], 2), own, number, TOK_DEV, SLOTS, TOPK, CAP, 2))(route_slot_keys, route_slot_turns).reshape((TOKENS, TOPK))
    gates = jnp.clip(0.2 + 0.8 * jax.random.uniform(part_splits[2], (TOKENS, TOPK), jnp.float32) ** levels(part_splits[2], (TOKENS, TOPK), ((0, 32),), -0.2, 0.2), 0.2, 1.0)
    gate_up = normal_values(key_of[3], (N_EA, D, 2 * HS), D ** -0.5, 0.0625, ((0, 32),))
    down = normal_values(key_of[4], (N_EA, HS, D), FF ** -0.5, 0.125, ((0, 32),))
    return {"tokens": tokens, "route_slot": route_slot, "gates": gates, "gate_up": gate_up, "down": down}


def reference(tokens, route_slot, gates, gate_up, down):
    pairs = TOKENS * TOPK
    flat_slot = route_slot.reshape(-1).astype(jnp.int32)
    flat_gate = gates.reshape(-1)
    owner = (jnp.arange(pairs, dtype=jnp.int32) // TOPK).astype(jnp.int32)
    order = jnp.argsort(flat_slot, stable=True).astype(jnp.int32)
    counts = jnp.sum((flat_slot[:, None] == jnp.arange(SLOTS, dtype=jnp.int32)[None, :]).astype(jnp.int32), axis=0)
    starts = (jnp.cumsum(counts) - counts).astype(jnp.int32)
    most_rows = N_EA * CAP

    def one_slot(total, slot):
        begin = jnp.minimum(starts[slot], pairs - most_rows).astype(jnp.int32)
        picked = lax.dynamic_slice_in_dim(order, begin, most_rows, 0)
        member = (flat_slot[picked] == slot)
        rows = tokens[owner[picked]]
        blocks = lax.dynamic_slice_in_dim(gate_up, (slot * TP).astype(jnp.int32), TP, 0)
        wide = jnp.transpose(blocks, (1, 0, 2)).reshape(D, TP * 2 * HS)
        both = jnp.dot(rows, wide, preferred_element_type=jnp.float32).reshape(most_rows, TP, 2 * HS)
        hidden = (jax.nn.silu(both[:, :, :HS]) * both[:, :, HS:]).astype(jnp.bfloat16).reshape(most_rows, FF)
        downs = lax.dynamic_slice_in_dim(down, (slot * TP).astype(jnp.int32), TP, 0).reshape(FF, D)
        result = jnp.dot(hidden, downs, preferred_element_type=jnp.float32)
        weight = jnp.where(member, flat_gate[picked], jnp.float32(0.0))
        total = total.at[owner[picked]].add(result * weight[:, None])
        return total, None

    total, unused = lax.scan(one_slot, jnp.zeros((TOKENS, D), jnp.float32), jnp.arange(SLOTS, dtype=jnp.int32))
    return total.astype(jnp.bfloat16)
```

```python
import jax
import jax.numpy as jnp
from jax import lax
from jax.sharding import PartitionSpec as P

TP = 8
LANES = 128
PIECES = 3


def from_partner(value, mask):
    return lax.ppermute(value, "ea", [(i, i ^ mask) for i in range(lax.axis_size("ea"))])


def gate_columns(route_slot, gates, slots):
    named = route_slot[:, :, None] == jnp.arange(slots, dtype=jnp.int32)[None, None, :]
    rest = jnp.sum(jnp.where(named, gates[:, :, None], 0.0), axis=1)
    pieces = []
    for _ in range(PIECES):
        piece = lax.reduce_precision(rest, 8, 7)
        pieces.append(piece)
        rest = rest - piece
    columns = jnp.concatenate(pieces, axis=1)
    padded = -(-columns.shape[1] // LANES) * LANES
    return jnp.pad(columns, ((0, 0), (0, padded - columns.shape[1]))).astype(jnp.bfloat16)


def own_gate(columns, slots, my_slot):
    lane = lax.broadcasted_iota(jnp.int32, columns.shape, 1)
    mine = (lane % slots == my_slot) & (lane < PIECES * slots)
    return jnp.sum(jnp.where(mine, columns.astype(jnp.float32), 0.0), axis=1, keepdims=True)


def gather(blocks, half):
    own = jnp.concatenate(blocks, axis=0)
    first = from_partner(own, 2)
    second = from_partner(own, 4)
    left = from_partner(second[:, :half], 2)
    right = from_partner(first[:, half:], 4)
    return [own, first, second, jnp.concatenate([left, right], axis=1)]


def scatter(parts, half):
    own, first, second, across = parts
    low = jnp.bfloat16
    left = from_partner(across[:, :half].astype(low), 2)
    right = from_partner(across[:, half:].astype(low), 4)
    second = jnp.concatenate([second[:, :half] + left, second[:, half:]], axis=1)
    first = jnp.concatenate([first[:, :half], first[:, half:] + right], axis=1)
    from_first = from_partner(first.astype(low), 2)
    from_second = from_partner(second.astype(low), 4)
    return own + from_first + from_second


def local(tokens, route_slot, gates, gate_up, down):
    rows, width = tokens.shape
    slots = lax.axis_size("ea") // TP
    my_slot = lax.axis_index("ea") // TP
    weights_in, weights_out = gate_up[0], down[0]
    hidden_width = weights_out.shape[0]
    half = width // LANES // 2 * LANES
    block = jnp.concatenate([tokens, gate_columns(route_slot, gates, slots)], axis=1)
    arrived = [block] + [from_partner(block, k * TP) for k in range(1, slots)]

    quads = gather(arrived, half)
    quad_rows = quads[0].shape[0]
    mine = jnp.concatenate(quads, axis=0)
    theirs = from_partner(mine, 1)
    both = jnp.concatenate([mine, theirs], axis=0)
    weight = own_gate(both[:, width:], slots, my_slot)
    product = jnp.dot(both[:, :width], weights_in, preferred_element_type=jnp.float32)
    hidden = (jax.nn.silu(product[:, :hidden_width]) * product[:, hidden_width:]).astype(jnp.bfloat16)
    result = jnp.dot(hidden, weights_out, preferred_element_type=jnp.float32) * weight
    split = mine.shape[0]
    kept = result[:split] + from_partner(result[split:].astype(jnp.bfloat16), 1)
    parts = [kept[i * quad_rows : (i + 1) * quad_rows] for i in range(4)]
    column = scatter(parts, half)
    total = column[:rows]
    for k in range(1, slots):
        total = total + from_partner(column[k * rows : (k + 1) * rows].astype(jnp.bfloat16), k * TP)
    return total.astype(jnp.bfloat16)


def solution(mesh):
    placed = (
        P(("ga", "ea"), None),
        P(("ga", "ea"), None),
        P(("ga", "ea"), None),
        P("ea", None, None),
        P("ea", None, None),
    )
    return jax.shard_map(
        local, mesh=mesh, in_specs=placed, out_specs=P(("ga", "ea"), None), check_vma=False
    )
```
